32 devices in a mesh: row: 8 (over y, x, core), col: 4 (over z).
Axes of the slice: x: 2, y: 2, z: 4, core: 2. Of those that a mesh axis runs over, the one named last changes fastest.
Arguments:
- features: bfloat16 [32768, 512], P('col', 'row'), may hold values from -6 to 6
- weight_t: bfloat16 [512, 512], P(None, 'row'), may hold values from -0.25 to 0.25
- tiles: bfloat16 [8192, 128, 128], P(('row', 'col')), may hold values from -0.15625 to 0.15625
- coords: int32 [2, 8192], P(None, ('row', 'col')), may hold values from 0 to 63, as said below
- counts: int32 [32], P(('row', 'col')), may hold values from 32 to 256, as said below
Outputs:
- output: bfloat16 [32768, 512], P('row', 'col')
The draws below stay inside these ranges and needn't reach their ends.
Inputs may be any that keep to these rules, and one draw needn't show every extreme that they name: coords[0] of a slot lies in 0 to 31 and coords[1] in 0 to 63; the live slots of one grid cell name distinct tiles. `counts`: some grid cell has all 256 slots live in every draw.
All inputs are finite; a program needn't handle non-finite values.
Results may differ from the reference program's by a relative error of at most 0.0095.
Values may be sent and summed in bfloat16 or wider, within the bound.
No kernel may reach another device: no remote copies, remote signals or barrier semaphores. Data moves between devices by JAX's collectives and lax.ppermute only.
A program may use at most 128 MiB of HBM per device.

```python
import jax
import jax.numpy as jnp
from jax import lax

TILE = 128
FEAT = 512
F_OUT = 512
TROW = 32
MAXT = 256
TCOL = 64
NODES = 32768
N_COL = 4
DEVICES = 32


def draw_coords(key, part):
    keys = jax.random.split(jax.random.fold_in(key, 11), DEVICES)
    spots = jax.vmap(lambda k: jax.random.permutation(k, TROW * TCOL)[:MAXT])(keys)
    spots = spots.reshape(DEVICES * MAXT).astype(jnp.int32)
    return jnp.stack([spots // TCOL, spots % TCOL]).astype(jnp.int32)


def draw_counts(key, part):
    base = jax.random.randint(jax.random.fold_in(key, 21), (DEVICES,), MAXT // 8, MAXT // 2 + 1)
    heavy = jax.random.randint(jax.random.fold_in(key, 22), (DEVICES,), 0, 8) == 0
    chosen = jax.random.randint(jax.random.fold_in(key, 23), (), 0, DEVICES)
    heavy = heavy | (jnp.arange(DEVICES, dtype=jnp.int32) == chosen)
    return jnp.where(heavy, MAXT, base).astype(jnp.int32)


def level_of(key, shape, cuts, least, high):
    level, own = 1.0, jax.random.fold_in(key, 6)
    for axis_at, parts in cuts:
        heights = jnp.exp(jax.random.uniform(jax.random.fold_in(own, axis_at), (parts,), jnp.float32, least / len(cuts), high / len(cuts)))
        level = level * jnp.repeat(heights, shape[axis_at] // parts).reshape([-1 if axis == axis_at else 1 for axis in range(len(shape))])
    return level


def scatter_about(key, dims, deviation, limit, pieces=(), kind=jnp.bfloat16):
    values = deviation * jax.random.normal(key, dims, jnp.float32)
    if pieces:
        values = values * level_of(key, dims, pieces, -0.22, 0.18)
    return jnp.clip(values, -limit, limit).astype(kind)


def setup_inputs(seed: int = 0) -> dict:
    streams_of = jax.random.split(jax.random.key(seed), 6)
    return {
        "features": scatter_about(streams_of[0], (NODES, FEAT), 1.0, 6.0, ((0, 4), (1, 8))),
        "weight_t": scatter_about(streams_of[1], (F_OUT, FEAT), FEAT ** -0.5, 0.25, ((1, 8),)),
        "tiles": scatter_about(streams_of[2], (DEVICES * MAXT, TILE, TILE), (2 * MAXT * TILE * N_COL // (5 * TROW)) ** -0.5, 0.15625, ((0, 32),)),
        "coords": draw_coords(jax.random.fold_in(streams_of[5], 71), 0),
        "counts": draw_counts(jax.random.fold_in(streams_of[5], 71), 0),
    }


def reference(features, weight_t, tiles, coords, counts):
    feat = features.shape[1]
    cblock = TCOL * TILE
    rblock = TROW * TILE
    lanes = jnp.arange(TROW, dtype=jnp.int32)
    slots = jnp.arange(MAXT, dtype=jnp.int32)

    def device(total, cell):
        rpos = cell // N_COL
        cpos = cell % N_COL
        block = lax.dynamic_slice_in_dim(tiles, (cell * MAXT).astype(jnp.int32), MAXT, 0).astype(jnp.float32)
        place = lax.dynamic_slice_in_dim(coords, (cell * MAXT).astype(jnp.int32), MAXT, 1)
        live = (slots < counts[cell]).astype(jnp.float32)
        panel = lax.dynamic_slice_in_dim(features, (cpos * cblock).astype(jnp.int32), cblock, 0)
        panel = panel.astype(jnp.float32).reshape(TCOL, TILE, feat)
        picked = panel[place[1]]
        prod = jnp.einsum('gij,gjw->giw', block * live[:, None, None], picked, precision=lax.Precision.HIGHEST)
        select = (place[0][:, None] == lanes[None, :]).astype(jnp.float32)
        part = jnp.einsum('gt,giw->tiw', select, prod, precision=lax.Precision.HIGHEST).reshape(rblock, feat)
        start = (rpos * rblock).astype(jnp.int32)
        old = lax.dynamic_slice_in_dim(total, start, rblock, 0)
        return lax.dynamic_update_slice_in_dim(total, old + part, start, 0), None

    total = jnp.zeros((NODES, feat), jnp.float32)
    total, _ = lax.scan(device, total, jnp.arange(DEVICES, dtype=jnp.int32))
    result = jnp.dot(total, weight_t.astype(jnp.float32).T, precision=lax.Precision.HIGHEST)
    return result.astype(jnp.bfloat16)
```

```python
import functools

import jax
import jax.numpy as jnp
from jax import lax
from jax.experimental import pallas as pl
from jax.experimental.pallas import tpu as pltpu
from jax.sharding import PartitionSpec as P

SPAN = 4
GROUP = 8
FEATURE_PARTS = 2
ROW_PARTS = 2


def plan_kernel(coords, counts, slot_out, col_out, row_out, edge_out, seen, begin, *, brows, pad_col):
    count = counts[0]
    jobs = row_out.shape[0]

    def clear(r, _):
        seen[r] = 0
        return 0

    lax.fori_loop(0, brows, clear, 0)

    def tally(s, _):
        r = coords[0, s]
        seen[r] = seen[r] + 1
        return 0

    lax.fori_loop(0, count, tally, 0)

    part_rows = brows // ROW_PARTS

    def blank(j, _):
        for k in range(SPAN):
            slot_out[j * SPAN + k] = 0
            col_out[j * SPAN + k] = pad_col
        row_out[j] = 0
        return 0

    lax.fori_loop(0, jobs, blank, 0)

    edge_out[0] = 0
    at = jnp.int32(0)
    for part in range(ROW_PARTS):

        def lay(r, at):
            begin[r] = at * SPAN
            return at + (seen[r] + SPAN - 1) // SPAN

        first = at
        at = lax.fori_loop(part * part_rows, (part + 1) * part_rows, lay, at)
        at = first + (at - first + GROUP - 1) // GROUP * GROUP
        edge_out[part + 1] = at // GROUP

    def place(s, _):
        r = coords[0, s]
        spot = begin[r]
        begin[r] = spot + 1
        slot_out[spot] = s
        col_out[spot] = coords[1, s]
        row_out[spot // SPAN] = r % part_rows
        return 0

    lax.fori_loop(0, count, place, 0)


def make_plan(coords, counts, brows, bcols):
    maxt = coords.shape[1]
    jobs = brows + -(-maxt // SPAN) + ROW_PARTS * GROUP
    jobs = -(-jobs // GROUP) * GROUP
    smem = pl.BlockSpec(memory_space=pltpu.SMEM)
    ints = lambda n: jax.ShapeDtypeStruct((n,), jnp.int32)
    return pl.pallas_call(
        functools.partial(plan_kernel, brows=brows, pad_col=bcols),
        out_shape=(ints(jobs * SPAN), ints(jobs * SPAN), ints(jobs), ints(ROW_PARTS + 1)),
        in_specs=[smem, smem],
        out_specs=(smem, smem, smem, smem),
        scratch_shapes=[pltpu.SMEM((brows,), jnp.int32), pltpu.SMEM((brows,), jnp.int32)],
        name="plan",
    )(coords, counts)


def apply_tiles(slot, col, row, edge, tiles, panel, acc, tbuf, pbuf, tsem, psem, lo, hi):
    tile = tiles.shape[1]
    per = GROUP * SPAN
    nodes = panel.shape[1]
    load = pltpu.make_async_copy(panel, pbuf.at[:, pl.ds(0, nodes)], psem)
    load.start()

    def fetch(g, _):
        for k in range(per):
            s = slot[g * per + k]
            pltpu.make_async_copy(
                tiles.at[s], tbuf.at[(g - lo) * per + k], tsem.at[g - lo]
            ).start()
        return 0

    lax.fori_loop(lo, hi, fetch, 0)
    pbuf[:, pl.ds(nodes, tile)] = jnp.zeros((pbuf.shape[0], tile), pbuf.dtype)
    acc[...] = jnp.zeros_like(acc)
    load.wait()

    def work(g, _):
        own = tbuf.at[pl.ds((g - lo) * per, per)]
        pltpu.make_async_copy(tiles.at[pl.ds(0, per)], own, tsem.at[g - lo]).wait()
        for j in range(GROUP):
            job = g * GROUP + j
            base = (g - lo) * per + j * SPAN
            lhs = jnp.concatenate([tbuf[base + k] for k in range(SPAN)], axis=1)
            rhs = jnp.concatenate(
                [
                    pbuf[:, pl.ds(pl.multiple_of(col[job * SPAN + k] * tile, tile), tile)]
                    for k in range(SPAN)
                ],
                axis=1,
            )
            prod = lax.dot_general(
                lhs, rhs, (((1,), (1,)), ((), ())), preferred_element_type=jnp.float32
            )
            spot = pl.ds(pl.multiple_of(row[job] * tile, tile), tile)
            acc[spot, :] = acc[spot, :] + prod
        return 0

    lax.fori_loop(lo, hi, work, 0)


def early_kernel(slot, col, row, edge, tiles, panel, out, acc, tbuf, pbuf, tsem, psem):
    rows = acc.shape[0]
    for part in range(ROW_PARTS):
        apply_tiles(
            slot, col, row, edge, tiles, panel, acc, tbuf, pbuf, tsem, psem,
            edge[part], edge[part + 1],
        )
        out[pl.ds(part * rows, rows), :] = acc[...].astype(out.dtype)


def last_kernel(slot, col, row, edge, tiles, panel, weight, *rest, part):
    *before, out, acc, tbuf, pbuf, tsem, psem = rest
    apply_tiles(
        slot, col, row, edge, tiles, panel, acc, tbuf, pbuf, tsem, psem,
        edge[part], edge[part + 1],
    )
    rows = acc.shape[0]
    step = min(rows, 512)
    for start in range(0, rows, step):
        spot = pl.ds(start, step)
        lhs = jnp.concatenate(
            [one[spot, :] for one in before] + [acc[spot, :].astype(jnp.bfloat16)], axis=1
        )
        out[spot, :] = jnp.dot(
            lhs, weight[...], preferred_element_type=jnp.float32
        ).astype(out.dtype)


def scratch_of(rows, width, nodes, tile, jobs):
    groups = jobs // GROUP
    return [
        pltpu.VMEM((rows, width), jnp.float32),
        pltpu.VMEM((jobs * SPAN, tile, tile), jnp.bfloat16),
        pltpu.VMEM((width, nodes + tile), jnp.bfloat16),
        pltpu.SemaphoreType.DMA((groups,)),
        pltpu.SemaphoreType.DMA,
    ]


def body(features, weight_t, tiles, coords, counts):
    maxt, tile, _ = tiles.shape
    nodes, wide = features.shape
    fout = weight_t.shape[0]
    nrow, ncol = lax.axis_size("row"), lax.axis_size("col")
    out_rows = nodes * ncol // nrow
    brows, bcols = out_rows // tile, nodes // tile
    piece = wide // FEATURE_PARTS
    width = piece * nrow
    rows = out_rows // ROW_PARTS

    plan = make_plan(coords, counts, brows, bcols)
    jobs = plan[2].shape[0]
    panels = []
    for f in range(FEATURE_PARTS):
        own = features[:, f * piece : (f + 1) * piece]
        if panels:
            own, _ = lax.optimization_barrier((own, own[:1]))
        panels.append(lax.all_gather(own, "row", axis=1, tiled=True).T)
    weight = lax.all_gather(weight_t, "row", axis=1, tiled=True).T
    weight = weight.reshape(nrow, FEATURE_PARTS, piece, fout).swapaxes(0, 1)
    weight = weight.reshape(FEATURE_PARTS * width, fout)

    smem = pl.BlockSpec(memory_space=pltpu.SMEM)
    hbm = pl.BlockSpec(memory_space=pl.ANY)
    scratch = scratch_of(rows, width, nodes, tile, jobs)
    limit = pltpu.CompilerParams(vmem_limit_bytes=48 * 1024 * 1024)
    flops = 2 * maxt * tile * tile * width
    before = [
        pl.pallas_call(
            early_kernel,
            out_shape=jax.ShapeDtypeStruct((out_rows, width), jnp.bfloat16),
            in_specs=[smem] * 4 + [hbm, hbm],
            scratch_shapes=scratch,
            compiler_params=limit,
            cost_estimate=pl.CostEstimate(flops=flops, transcendentals=0, bytes_accessed=1 << 24),
            name="early",
        )(*plan, tiles, panel)
        for panel in panels[:-1]
    ]
    outs = []
    for part in range(ROW_PARTS):
        here = pl.BlockSpec((rows, width), lambda i, part=part: (part, 0))
        partial = pl.pallas_call(
            functools.partial(last_kernel, part=part),
            grid=(1,),
            out_shape=jax.ShapeDtypeStruct((rows, fout), jnp.bfloat16),
            in_specs=[smem] * 4
            + [hbm, hbm, pl.BlockSpec(weight.shape, lambda i: (0, 0))]
            + [here] * len(before),
            out_specs=pl.BlockSpec((rows, fout), lambda i: (0, 0)),
            scratch_shapes=scratch,
            compiler_params=limit,
            cost_estimate=pl.CostEstimate(flops=flops, transcendentals=0, bytes_accessed=1 << 24),
            name="last",
        )(*plan, tiles, panels[-1], weight, *before)
        outs.append(lax.psum_scatter(partial, "col", scatter_dimension=1, tiled=True))
    return jnp.concatenate(outs, axis=0).astype(jnp.bfloat16)


def solution(mesh):
    placed = (
        P("col", "row"),
        P(None, "row"),
        P(("row", "col"), None, None),
        P(None, ("row", "col")),
        P(("row", "col")),
    )
    return jax.shard_map(
        body, mesh=mesh, in_specs=placed, out_specs=P("row", "col"), check_vma=False
    )
```

```python
import functools

import jax
import jax.numpy as jnp
from jax import lax
from jax.experimental import pallas as pl
from jax.experimental.pallas import tpu as pltpu
from jax.sharding import PartitionSpec as P

SPAN = 4
GROUP = 8


def row_cuts(brows):
    return (0, max(brows // 4, 1), brows)


def plan_kernel(coords, counts, slot_out, col_out, row_out, edge_out, seen, begin, *, brows, pad_col):
    count = counts[0]
    jobs = row_out.shape[0]

    def clear(r, _):
        seen[r] = 0
        return 0

    lax.fori_loop(0, brows, clear, 0)

    def tally(s, _):
        r = coords[0, s]
        seen[r] = seen[r] + 1
        return 0

    lax.fori_loop(0, count, tally, 0)

    cuts = row_cuts(brows)

    def blank(j, _):
        for k in range(SPAN):
            slot_out[j * SPAN + k] = 0
            col_out[j * SPAN + k] = pad_col
        row_out[j] = 0
        return 0

    lax.fori_loop(0, jobs, blank, 0)

    edge_out[0] = 0
    at = jnp.int32(0)
    for part in range(len(cuts) - 1):

        def lay(r, at):
            begin[r] = at * SPAN
            return at + (seen[r] + SPAN - 1) // SPAN

        first = at
        at = lax.fori_loop(cuts[part], cuts[part + 1], lay, at)
        at = first + (at - first + GROUP - 1) // GROUP * GROUP
        edge_out[part + 1] = at // GROUP

    def place(s, _):
        r = coords[0, s]
        spot = begin[r]
        begin[r] = spot + 1
        slot_out[spot] = s
        col_out[spot] = coords[1, s]
        row_out[spot // SPAN] = r
        return 0

    lax.fori_loop(0, count, place, 0)


def make_plan(coords, counts, brows, bcols):
    maxt = coords.shape[1]
    parts = len(row_cuts(brows)) - 1
    jobs = brows + -(-maxt // SPAN) + parts * GROUP
    jobs = -(-jobs // GROUP) * GROUP
    smem = pl.BlockSpec(memory_space=pltpu.SMEM)
    ints = lambda n: jax.ShapeDtypeStruct((n,), jnp.int32)
    return pl.pallas_call(
        functools.partial(plan_kernel, brows=brows, pad_col=bcols),
        out_shape=(ints(jobs * SPAN), ints(jobs * SPAN), ints(jobs), ints(parts + 1)),
        in_specs=[smem, smem],
        out_specs=(smem, smem, smem, smem),
        scratch_shapes=[pltpu.SMEM((brows,), jnp.int32), pltpu.SMEM((brows,), jnp.int32)],
        name="plan",
    )(coords, counts)


def apply_tiles(slot, col, row, edge, tiles, panel, acc, tbuf, pbuf, tsem, psem, lo, hi, first):
    tile = tiles.shape[1]
    per = GROUP * SPAN
    nodes = panel.shape[1]
    load = pltpu.make_async_copy(panel, pbuf.at[:, pl.ds(0, nodes)], psem)
    load.start()

    def fetch(g, _):
        for k in range(per):
            s = slot[g * per + k]
            pltpu.make_async_copy(
                tiles.at[s], tbuf.at[(g - lo) * per + k], tsem.at[g - lo]
            ).start()
        return 0

    lax.fori_loop(lo, hi, fetch, 0)
    pbuf[:, pl.ds(nodes, tile)] = jnp.zeros((pbuf.shape[0], tile), pbuf.dtype)
    acc[...] = jnp.zeros_like(acc)
    load.wait()

    def work(g, _):
        own = tbuf.at[pl.ds((g - lo) * per, per)]
        pltpu.make_async_copy(tiles.at[pl.ds(0, per)], own, tsem.at[g - lo]).wait()
        for j in range(GROUP):
            job = g * GROUP + j
            base = (g - lo) * per + j * SPAN
            lhs = jnp.concatenate([tbuf[base + k] for k in range(SPAN)], axis=1)
            rhs = jnp.concatenate(
                [
                    pbuf[:, pl.ds(pl.multiple_of(col[job * SPAN + k] * tile, tile), tile)]
                    for k in range(SPAN)
                ],
                axis=1,
            )
            prod = lax.dot_general(
                lhs, rhs, (((1,), (1,)), ((), ())), preferred_element_type=jnp.float32
            )
            spot = pl.ds(pl.multiple_of(jnp.maximum(row[job] - first, 0) * tile, tile), tile)
            acc[spot, :] = acc[spot, :] + prod
        return 0

    lax.fori_loop(lo, hi, work, 0)


def part_kernel(slot, col, row, edge, tiles, panel, weight, out, acc, tbuf, pbuf, tsem, psem, *, part, first):
    apply_tiles(
        slot, col, row, edge, tiles, panel, acc, tbuf, pbuf, tsem, psem,
        edge[part], edge[part + 1], first,
    )
    rows = acc.shape[0]
    ncol, _, fout = out.shape
    step = next(n for n in (512, 256, 128, rows) if rows % n == 0)
    for start in range(0, rows, step):
        spot = pl.ds(start, step)
        done = jnp.dot(
            acc[spot, :].astype(jnp.bfloat16), weight[...], preferred_element_type=jnp.float32
        ).astype(out.dtype)
        for c in range(ncol):
            out[c, spot, :] = done[:, c * fout : (c + 1) * fout]


def body(features, weight_t, tiles, coords, counts):
    maxt, tile, _ = tiles.shape
    nodes, wide = features.shape
    fout = weight_t.shape[0]
    nrow, ncol = lax.axis_size("row"), lax.axis_size("col")
    brows, bcols = nodes * ncol // nrow // tile, nodes // tile
    width = wide * nrow

    plan = make_plan(coords, counts, brows, bcols)
    jobs = plan[2].shape[0]
    panel = lax.all_gather(features, "row", axis=1, tiled=True).T
    weight = lax.all_gather(weight_t, "row", axis=1, tiled=True).T

    smem = pl.BlockSpec(memory_space=pltpu.SMEM)
    hbm = pl.BlockSpec(memory_space=pl.ANY)
    cuts = row_cuts(brows)
    outs = []
    for part, (low, high) in enumerate(zip(cuts[:-1], cuts[1:])):
        rows = (high - low) * tile
        shape = (ncol, rows, fout // ncol)
        partial = pl.pallas_call(
            functools.partial(part_kernel, part=part, first=low),
            grid=(1,),
            out_shape=jax.ShapeDtypeStruct(shape, jnp.bfloat16),
            in_specs=[smem] * 4 + [hbm, hbm, pl.BlockSpec(weight.shape, lambda i: (0, 0))],
            out_specs=pl.BlockSpec(shape, lambda i: (0, 0, 0)),
            scratch_shapes=[
                pltpu.VMEM((rows, width), jnp.float32),
                pltpu.VMEM((jobs * SPAN, tile, tile), jnp.bfloat16),
                pltpu.VMEM((width, nodes + tile), jnp.bfloat16),
                pltpu.SemaphoreType.DMA((jobs // GROUP,)),
                pltpu.SemaphoreType.DMA,
            ],
            compiler_params=pltpu.CompilerParams(vmem_limit_bytes=52 * 1024 * 1024),
            cost_estimate=pl.CostEstimate(
                flops=2 * maxt * tile * tile * width, transcendentals=0, bytes_accessed=1 << 24
            ),
            name="part",
        )(*plan, tiles, panel, weight)
        outs.append(lax.psum_scatter(partial, "col", scatter_dimension=0, tiled=False))
    return jnp.concatenate(outs, axis=0)


def solution(mesh):
    placed = (
        P("col", "row"),
        P(None, "row"),
        P(("row", "col"), None, None),
        P(None, ("row", "col")),
        P(("row", "col")),
    )
    return jax.shard_map(
        body, mesh=mesh, in_specs=placed, out_specs=P("row", "col"), check_vma=False
    )
```

```python
import functools

import jax
import jax.numpy as jnp
from jax import lax
from jax.experimental import pallas as pl
from jax.experimental.pallas import tpu as pltpu
from jax.sharding import PartitionSpec as P

SPAN = 4
GROUP = 8


def row_cuts(brows):
    return (0, max(brows // 4, 1), brows)


def table_spots(jobs):
    return 0, jobs * SPAN, 2 * jobs * SPAN, (2 * SPAN + 1) * jobs


def plan_kernel(coords, counts, table, seen, begin, *, brows, pad_col, jobs):
    count = counts[0]
    slot_at, col_at, row_at, edge_at = table_spots(jobs)

    def clear(r, _):
        seen[r] = 0
        return 0

    lax.fori_loop(0, brows, clear, 0)

    def tally(s, _):
        r = coords[0, s]
        seen[r] = seen[r] + 1
        return 0

    lax.fori_loop(0, count, tally, 0)

    cuts = row_cuts(brows)

    def blank(j, _):
        for k in range(SPAN):
            table[slot_at + j * SPAN + k] = 0
            table[col_at + j * SPAN + k] = pad_col
        table[row_at + j] = 0
        return 0

    lax.fori_loop(0, jobs, blank, 0)

    table[edge_at] = 0
    at = jnp.int32(0)
    for part in range(len(cuts) - 1):

        def lay(r, at):
            begin[r] = at * SPAN
            return at + (seen[r] + SPAN - 1) // SPAN

        first = at
        at = lax.fori_loop(cuts[part], cuts[part + 1], lay, at)
        at = first + (at - first + GROUP - 1) // GROUP * GROUP
        table[edge_at + part + 1] = at // GROUP

    def place(s, _):
        r = coords[0, s]
        spot = begin[r]
        begin[r] = spot + 1
        table[slot_at + spot] = s
        table[col_at + spot] = coords[1, s]
        table[row_at + spot // SPAN] = r
        return 0

    lax.fori_loop(0, count, place, 0)


def make_plan(coords, counts, brows, bcols):
    maxt = coords.shape[1]
    parts = len(row_cuts(brows)) - 1
    jobs = brows + -(-maxt // SPAN) + parts * GROUP
    jobs = -(-jobs // GROUP) * GROUP
    smem = pl.BlockSpec(memory_space=pltpu.SMEM)
    size = table_spots(jobs)[-1] + parts + 1
    table = pl.pallas_call(
        functools.partial(plan_kernel, brows=brows, pad_col=bcols, jobs=jobs),
        out_shape=jax.ShapeDtypeStruct((size,), jnp.int32),
        in_specs=[smem, smem],
        out_specs=smem,
        scratch_shapes=[pltpu.SMEM((brows,), jnp.int32), pltpu.SMEM((brows,), jnp.int32)],
        name="plan",
    )(coords, counts)
    return table, jobs


def apply_tiles(table, jobs, tiles, panel, acc, tbuf, pbuf, tsem, psem, part, first):
    slot_at, col_at, row_at, edge_at = table_spots(jobs)
    lo, hi = table[edge_at + part], table[edge_at + part + 1]
    tile = tiles.shape[1]
    per = GROUP * SPAN
    nodes = panel.shape[1]
    half = panel.shape[0] // 2
    loads = [
        pltpu.make_async_copy(
            panel.at[pl.ds(h * half, half)],
            pbuf.at[pl.ds(h * half, half), pl.ds(0, nodes)],
            psem.at[h],
        )
        for h in range(2)
    ]
    loads[0].start()

    def fetch(g, _):
        for k in range(per):
            s = table[slot_at + g * per + k]
            pltpu.make_async_copy(
                tiles.at[s], tbuf.at[(g - lo) * per + k], tsem.at[g - lo]
            ).start()
        return 0

    lax.fori_loop(lo, hi, fetch, 0)
    loads[1].start()
    pbuf[:, pl.ds(nodes, tile)] = jnp.zeros((pbuf.shape[0], tile), pbuf.dtype)
    acc[...] = jnp.zeros_like(acc)

    def work(g, _, h):
        own = tbuf.at[pl.ds((g - lo) * per, per)]
        if h == 0:
            pltpu.make_async_copy(tiles.at[pl.ds(0, per)], own, tsem.at[g - lo]).wait()
        side = pl.ds(h * half, half)
        for j in range(GROUP):
            job = g * GROUP + j
            base = (g - lo) * per + j * SPAN
            lhs = jnp.concatenate([tbuf[base + k] for k in range(SPAN)], axis=1)
            cols = [
                pl.ds(pl.multiple_of(table[col_at + job * SPAN + k] * tile, tile), tile)
                for k in range(SPAN)
            ]
            rhs = jnp.concatenate([pbuf[side, col] for col in cols], axis=1)
            prod = lax.dot_general(
                lhs, rhs, (((1,), (1,)), ((), ())), preferred_element_type=jnp.float32
            )
            at = jnp.maximum(table[row_at + job] - first, 0) * tile
            spot = pl.ds(pl.multiple_of(at, tile), tile)
            acc[spot, side] = acc[spot, side] + prod
        return 0

    for h in range(2):
        loads[h].wait()
        lax.fori_loop(lo, hi, functools.partial(work, h=h), 0)


def part_kernel(table, tiles, panel, weight, out, acc, tbuf, pbuf, tsem, psem, *, jobs, part, first):
    apply_tiles(
        table, jobs, tiles, panel, acc, tbuf, pbuf, tsem, psem, part, first
    )
    rows = acc.shape[0]
    ncol, _, fout = out.shape
    step = next(n for n in (512, 256, 128, rows) if rows % n == 0)
    for start in range(0, rows, step):
        spot = pl.ds(start, step)
        done = jnp.dot(
            acc[spot, :].astype(jnp.bfloat16), weight[...], preferred_element_type=jnp.float32
        ).astype(out.dtype)
        for c in range(ncol):
            out[c, spot, :] = done[:, c * fout : (c + 1) * fout]


def body(features, weight_t, tiles, coords, counts):
    maxt, tile, _ = tiles.shape
    nodes, wide = features.shape
    fout = weight_t.shape[0]
    nrow, ncol = lax.axis_size("row"), lax.axis_size("col")
    brows, bcols = nodes * ncol // nrow // tile, nodes // tile
    width = wide * nrow

    table, jobs = make_plan(coords, counts, brows, bcols)
    panel = lax.all_gather(features, "row", axis=1, tiled=True).T
    weight = lax.all_gather(weight_t, "row", axis=1, tiled=True).T

    smem = pl.BlockSpec(memory_space=pltpu.SMEM)
    hbm = pl.BlockSpec(memory_space=pl.ANY)
    cuts = row_cuts(brows)
    outs = []
    for part, (low, high) in enumerate(zip(cuts[:-1], cuts[1:])):
        rows = (high - low) * tile
        shape = (ncol, rows, fout // ncol)
        partial = pl.pallas_call(
            functools.partial(part_kernel, jobs=jobs, part=part, first=low),
            grid=(1,),
            out_shape=jax.ShapeDtypeStruct(shape, jnp.bfloat16),
            in_specs=[smem, hbm, hbm, pl.BlockSpec(weight.shape, lambda i: (0, 0))],
            out_specs=pl.BlockSpec(shape, lambda i: (0, 0, 0)),
            scratch_shapes=[
                pltpu.VMEM((rows, width), jnp.float32),
                pltpu.VMEM((jobs * SPAN, tile, tile), jnp.bfloat16),
                pltpu.VMEM((width, nodes + tile), jnp.bfloat16),
                pltpu.SemaphoreType.DMA((jobs // GROUP,)),
                pltpu.SemaphoreType.DMA((2,)),
            ],
            compiler_params=pltpu.CompilerParams(vmem_limit_bytes=52 * 1024 * 1024),
            cost_estimate=pl.CostEstimate(
                flops=2 * maxt * tile * tile * width, transcendentals=0, bytes_accessed=1 << 24
            ),
            name="part",
        )(table, tiles, panel, weight)
        outs.append(lax.psum_scatter(partial, "col", scatter_dimension=0, tiled=False))
    return jnp.concatenate(outs, axis=0)


def solution(mesh):
    placed = (
        P("col", "row"),
        P(None, "row"),
        P(("row", "col"), None, None),
        P(None, ("row", "col")),
        P(("row", "col")),
    )
    return jax.shard_map(
        body, mesh=mesh, in_specs=placed, out_specs=P("row", "col"), check_vma=False
    )
```
